32 devices in a mesh: depth: 4 (over z), row: 2 (over x), col: 4 (over y, core).
Axes of the slice: x: 2, y: 2, z: 4, core: 2. Of those that a mesh axis runs over, the one named last changes fastest.
Arguments:
- tokens: bfloat16 [192, 8192], P('row', ('depth', 'col')), may hold values from -6 to 6
- cotangent: bfloat16 [192, 8192], P('row', ('depth', 'col')), may hold values from -1.609375 to 1.609375
- gate_weight: bfloat16 [8192, 14336], P(('depth', 'col'), 'row'), may hold values from -0.0625 to 0.0625
- up_weight: bfloat16 [8192, 14336], P(('depth', 'col'), 'row'), may hold values from -0.0625 to 0.0625
- down_weight: bfloat16 [14336, 8192], P('row', ('depth', 'col')), may hold values from -0.046875 to 0.046875
Outputs:
- input_grad: bfloat16 [192, 8192], P('row', ('depth', 'col'))
- gate_grad: bfloat16 [8192, 14336], P(('depth', 'col'), 'row')
- up_grad: bfloat16 [8192, 14336], P(('depth', 'col'), 'row')
- down_grad: bfloat16 [14336, 8192], P('row', ('depth', 'col'))
The draws below stay inside these ranges and needn't reach their ends.
All inputs are finite; a program needn't handle non-finite values.
Results may differ from the reference program's by a relative error of at most 0.0065.
Values may be sent and summed in bfloat16 or wider, within the bound.
No kernel may reach another device: no remote copies, remote signals or barrier semaphores. Data moves between devices by JAX's collectives and lax.ppermute only.
A program may use at most 128 MiB of HBM per device.

```python
import jax
import jax.numpy as jnp
from jax import lax

D = 8192
FF = 14336
TOKENS = 192


def block_levels(stream_key, dims, shards, smallest, largest):
    factor_of = 1.0
    for dim, parts in shards:
        heights = jax.random.uniform(jax.random.fold_in(jax.random.fold_in(stream_key, 6), dim), (parts,), jnp.float32, smallest / len(shards), largest / len(shards))
        factor_of = factor_of * jnp.repeat(jnp.exp(heights), dims[dim] // parts).reshape((-1,) + (1,) * (len(dims) - 1 - dim))
    return factor_of


def centred(stream_key, dims, width, bound, pieces=(), kind=jnp.bfloat16):
    array = width * jax.random.normal(stream_key, dims, jnp.float32)
    if pieces:
        array = array * block_levels(stream_key, dims, pieces, -0.22, 0.18)
    return jnp.clip(array, -bound, bound).astype(kind)


def setup_inputs(seed: int = 0) -> dict:
    arg_keys = jax.random.split(jax.random.key(seed), 6)
    return {
        "tokens": centred(arg_keys[0], (TOKENS, D), 1.0, 6.0, ((0, 2), (1, 16))),
        "cotangent": centred(arg_keys[1], (TOKENS, D), (TOKENS ** -0.25), 1.609375, ((0, 2), (1, 16))),
        "gate_weight": centred(arg_keys[2], (D, FF), D ** -0.5, 0.0625, ((0, 16), (1, 2))),
        "up_weight": centred(arg_keys[3], (D, FF), D ** -0.5, 0.0625, ((0, 16), (1, 2))),
        "down_weight": centred(arg_keys[4], (FF, D), FF ** -0.5, 0.046875, ((0, 2), (1, 16))),
    }


def reference(tokens, cotangent, gate_weight, up_weight, down_weight):
    gate = jnp.dot(tokens, gate_weight, preferred_element_type=jnp.float32)
    up = jnp.dot(tokens, up_weight, preferred_element_type=jnp.float32)
    back = lax.dot_general(cotangent, down_weight, (((1,), (1,)), ((), ())), preferred_element_type=jnp.float32)
    sig = jax.nn.sigmoid(gate)
    hidden = (gate * sig * up).astype(jnp.bfloat16)
    grad_gate = (back * up * sig * (1.0 + gate * (1.0 - sig))).astype(jnp.bfloat16)
    grad_up = (back * gate * sig).astype(jnp.bfloat16)
    input_grad = lax.dot_general(grad_gate, gate_weight, (((1,), (1,)), ((), ())), preferred_element_type=jnp.float32)
    input_grad = input_grad + lax.dot_general(grad_up, up_weight, (((1,), (1,)), ((), ())), preferred_element_type=jnp.float32)
    gate_grad = lax.dot_general(tokens, grad_gate, (((0,), (0,)), ((), ())), preferred_element_type=jnp.float32)
    up_grad = lax.dot_general(tokens, grad_up, (((0,), (0,)), ((), ())), preferred_element_type=jnp.float32)
    down_grad = lax.dot_general(hidden, cotangent, (((0,), (0,)), ((), ())), preferred_element_type=jnp.float32)
    return (input_grad.astype(jnp.bfloat16), gate_grad.astype(jnp.bfloat16),
            up_grad.astype(jnp.bfloat16), down_grad.astype(jnp.bfloat16))
```

```python
import jax
import jax.numpy as jnp
from jax import lax
from jax.experimental import pallas as pl
from jax.experimental.pallas import tpu as pltpu
from jax.sharding import PartitionSpec as P

LANES = 128
MIB = 1 << 20
F32 = jnp.float32
BF16 = jnp.bfloat16


def swiglu_back(gate, up, back):
    sig = jax.nn.sigmoid(gate)
    hidden = (gate * sig * up).astype(jnp.bfloat16)
    grad_gate = (back * up * sig * (1.0 + gate * (1.0 - sig))).astype(jnp.bfloat16)
    grad_up = (back * gate * sig).astype(jnp.bfloat16)
    return (hidden, grad_gate, grad_up)


def contract_rows(left, right):
    return lax.dot_general(
        left, right, (((0,), (0,)), ((), ())), preferred_element_type=jnp.float32
    )


def contract_cols(left, right):
    return lax.dot_general(
        left, right, (((1,), (1,)), ((), ())), preferred_element_type=jnp.float32
    )


def stationary(tokens, cotangent, gate_weight, up_weight, down_weight):
    rows_all, cot_all = (
        lax.all_gather(tokens, "row", axis=0, tiled=True),
        lax.all_gather(cotangent, "row", axis=0, tiled=True),
    )
    width = gate_weight.shape[1]
    gate_part = jnp.dot(rows_all, gate_weight, preferred_element_type=jnp.float32)
    up_part = jnp.dot(rows_all, up_weight, preferred_element_type=jnp.float32)
    back_part = contract_cols(cot_all, down_weight)
    summed = lax.psum_scatter(
        jnp.concatenate([gate_part, up_part, back_part], axis=1),
        ("depth", "col"),
        scatter_dimension=0,
        tiled=True,
    )
    hidden, grad_gate, grad_up = swiglu_back(
        summed[:, :width], summed[:, width : 2 * width], summed[:, 2 * width :]
    )
    hidden_piece = lax.all_gather(hidden, ("depth", "col"), axis=0, tiled=True)
    gate_piece = lax.all_gather(grad_gate, ("depth", "col"), axis=0, tiled=True)
    up_piece = lax.all_gather(grad_up, ("depth", "col"), axis=0, tiled=True)
    acc_gate = contract_rows(rows_all, gate_piece)
    acc_up = contract_rows(rows_all, up_piece)
    acc_down = contract_rows(hidden_piece, cot_all)
    block = contract_cols(gate_piece, gate_weight) + contract_cols(up_piece, up_weight)
    input_grad = lax.psum_scatter(block, "row", scatter_dimension=0, tiled=True)
    return tuple(a.astype(BF16) for a in (input_grad, acc_gate, acc_up, acc_down))


def swap(value, axis, mask, size):
    return lax.ppermute(value, axis, [(i, i ^ mask) for i in range(size)])


VMEM = pl.BlockSpec(memory_space=pltpu.VMEM)


def near(*arrays):
    return tuple(pltpu.with_memory_space_constraint(a, pltpu.VMEM) for a in arrays)


def estimate(flops, moved):
    return pl.CostEstimate(flops=flops, bytes_accessed=moved, transcendentals=0)


def order_kernel(where_ref, t_ref, c_ref, tp_ref, cp_ref, tt_ref):
    rows = t_ref.shape[0] // 4
    for q in range(4):
        start = pl.multiple_of((where_ref[1] ^ q) * rows, 16)
        tp_ref[q * rows : (q + 1) * rows, :] = t_ref[pl.ds(start, rows), :]
        cp_ref[q * rows : (q + 1) * rows, :] = c_ref[pl.ds(start, rows), :]
    tt_ref[...] = tp_ref[...].T


def order_rows(where, tokens, cot):
    n, d = tokens.shape
    return pl.pallas_call(
        order_kernel,
        in_specs=[pl.BlockSpec(memory_space=pltpu.SMEM), VMEM, VMEM],
        out_specs=[VMEM] * 3,
        out_shape=[
            pltpu.VMEM((n, d), BF16),
            pltpu.VMEM((n, d), BF16),
            pltpu.VMEM((d, n), BF16),
        ],
        cost_estimate=estimate(1 << 20, 5 * n * d * 2),
        compiler_params=pltpu.CompilerParams(vmem_limit_bytes=4 * MIB),
        name="order_rows",
    )(where, *near(tokens, cot))


def project_kernel(where_ref, t_ref, c_ref, wg_ref, wu_ref, wd_ref, keep_ref, send_ref):
    rows = t_ref.shape[0] // 4
    k = pl.program_id(0)
    tokens = t_ref[...]
    products = (
        lambda: jnp.dot(tokens, wg_ref[...], preferred_element_type=F32),
        lambda: jnp.dot(tokens, wu_ref[...], preferred_element_type=F32),
        lambda: contract_cols(c_ref[...], wd_ref[...]),
    )
    for i, product in enumerate(products):
        value = product()
        for y in range(2):
            keep_ref[k, y, i] = value[2 * y * rows : (2 * y + 1) * rows]
            send_ref[k, y, i] = value[(2 * y + 1) * rows : (2 * y + 2) * rows].astype(BF16)


def project(where, tokens, cot, gate_weight, up_weight, down_weight, base, width):
    n, d = tokens.shape
    rows = n // 4
    first = base // width
    columns = pl.BlockSpec((d, width), lambda k, s: (0, first + (s[0] ^ k)))
    down = pl.BlockSpec((width, d), lambda k, s: (first + (s[0] ^ k), 0))
    shape = (4, 2, 3, rows, width)
    return pl.pallas_call(
        project_kernel,
        grid_spec=pltpu.PrefetchScalarGridSpec(
            num_scalar_prefetch=1,
            grid=(4,),
            in_specs=[VMEM, VMEM, columns, columns, down],
            out_specs=[VMEM, VMEM],
        ),
        out_shape=[pltpu.VMEM(shape, F32), pltpu.VMEM(shape, BF16)],
        cost_estimate=estimate(6 * n * d * 4 * width, 3 * d * 4 * width * 2),
        compiler_params=pltpu.CompilerParams(vmem_limit_bytes=12 * MIB),
        name="project",
    )(where, *near(tokens, cot), gate_weight, up_weight, down_weight)


def halve_kernel(kept_ref, got_ref, keep_ref, send_ref):
    major, _, minor = kept_ref.shape[:3]

    @pl.loop(0, major * minor)
    def _(i):
        a, b = i // minor, i % minor
        keep_ref[a, b] = kept_ref[a, 0, b] + got_ref[a, 0, b].astype(F32)
        send_ref[a, b] = (kept_ref[a, 1, b] + got_ref[a, 1, b].astype(F32)).astype(BF16)


def halve(kept, got, major):
    r, w = kept.shape[-2:]
    minor = kept.size // (2 * major * r * w)
    kept = kept.reshape(major, 2, minor, r, w)
    got = got.reshape(major, 2, minor, r, w)
    shape = (major, minor, r, w)
    return pl.pallas_call(
        halve_kernel,
        in_specs=[VMEM, VMEM],
        out_specs=[VMEM, VMEM],
        out_shape=[pltpu.VMEM(shape, F32), pltpu.VMEM(shape, BF16)],
        cost_estimate=estimate(kept.size, kept.size * 9),
        compiler_params=pltpu.CompilerParams(vmem_limit_bytes=4 * MIB),
        name="halve",
    )(*near(kept, got))


def gate_kernel(kept_ref, got_ref, out_ref):
    gate, up, back = (kept_ref[i] + got_ref[i].astype(F32) for i in range(3))
    for i, value in enumerate(swiglu_back(gate, up, back)):
        out_ref[i] = value


def gate_rule(kept, got):
    return pl.pallas_call(
        gate_kernel,
        in_specs=[VMEM, VMEM],
        out_specs=VMEM,
        out_shape=pltpu.VMEM(kept.shape, BF16),
        cost_estimate=estimate(kept.size * 10, kept.size * 8),
        compiler_params=pltpu.CompilerParams(vmem_limit_bytes=4 * MIB),
        name="gate_rule",
    )(*near(kept, got))


def stack_kernel(*refs):
    for i, ref in enumerate(refs[:-1]):
        refs[-1][i] = ref[...]


def stack_blocks(*blocks):
    shape = (len(blocks), *blocks[0].shape)
    return pl.pallas_call(
        stack_kernel,
        in_specs=[VMEM] * len(blocks),
        out_specs=VMEM,
        out_shape=pltpu.VMEM(shape, BF16),
        cost_estimate=estimate(1 << 16, 16 * blocks[0].size),
        compiler_params=pltpu.CompilerParams(vmem_limit_bytes=4 * MIB),
        name="stack_blocks",
    )(*near(*blocks))


def rows_of(refs, i):
    k = pl.program_id(0)
    return jnp.concatenate([ref[k, i] for ref in refs], axis=0)


def input_kernel(where_ref, *refs):
    shares, (wg_ref, wu_ref, before_ref), (total_ref,) = refs[:4], refs[4:7], refs[7:]

    @pl.when(pl.program_id(0) == 0)
    def _():
        total_ref[...] = before_ref[...]

    total_ref[...] += contract_cols(rows_of(shares, 1), wg_ref[...]) + contract_cols(
        rows_of(shares, 2), wu_ref[...]
    )


def input_part(where, shares, gate_weight, up_weight, before, base, width):
    n, d = before.shape
    first = base // width
    columns = pl.BlockSpec((d, width), lambda k, s: (0, first + (s[0] ^ k)))
    return pl.pallas_call(
        input_kernel,
        grid_spec=pltpu.PrefetchScalarGridSpec(
            num_scalar_prefetch=1,
            grid=(4,),
            in_specs=[VMEM] * 4 + [columns, columns, VMEM],
            out_specs=VMEM,
        ),
        out_shape=pltpu.VMEM((n, d), F32),
        cost_estimate=estimate(4 * n * d * 4 * width, 2 * d * 4 * width * 2),
        compiler_params=pltpu.CompilerParams(vmem_limit_bytes=12 * MIB),
        name="input_part",
    )(where, *near(*shares), gate_weight, up_weight, *near(before))


def weight_kernel(where_ref, *refs):
    shares, (tt_ref, c_ref) = refs[:4], refs[4:6]
    gate_ref, up_ref, down_ref = refs[-3:]
    tokens = tt_ref[...]
    gate_ref[...] = jnp.dot(tokens, rows_of(shares, 1), preferred_element_type=F32).astype(BF16)
    up_ref[...] = jnp.dot(tokens, rows_of(shares, 2), preferred_element_type=F32).astype(BF16)
    down_ref[...] = contract_rows(rows_of(shares, 0), c_ref[...]).astype(BF16)


def weight_part(where, shares, tokens_t, cot, grads, shapes, base, width):
    n, d = cot.shape
    first = base // width
    columns = pl.BlockSpec((d, width), lambda k, s: (0, first + (s[0] ^ k)))
    down = pl.BlockSpec((width, d), lambda k, s: (first + (s[0] ^ k), 0))
    in_specs = [VMEM] * 6
    aliases = {}
    if grads:
        in_specs += [pl.BlockSpec(memory_space=pl.ANY)] * 3
        aliases = {7: 0, 8: 1, 9: 2}
    return pl.pallas_call(
        weight_kernel,
        grid_spec=pltpu.PrefetchScalarGridSpec(
            num_scalar_prefetch=1,
            grid=(4,),
            in_specs=in_specs,
            out_specs=[columns, columns, down],
        ),
        out_shape=[jax.ShapeDtypeStruct(s, BF16) for s in shapes],
        input_output_aliases=aliases,
        cost_estimate=estimate(6 * n * d * 4 * width, 3 * d * 4 * width * 2),
        compiler_params=pltpu.CompilerParams(vmem_limit_bytes=14 * MIB),
        name="weight_part",
    )(where, *near(*shares, tokens_t, cot), *grads)


def split_kernel(where_ref, total_ref, keep_ref, send_ref):
    rows = total_ref.shape[0] // 4
    row, col = where_ref[2], where_ref[1]
    for i in range(2):
        mine = pl.multiple_of((col ^ (2 * row + i)) * rows, 16)
        other = pl.multiple_of((col ^ (2 * (1 - row) + i)) * rows, 16)
        keep_ref[i * rows : (i + 1) * rows, :] = total_ref[pl.ds(mine, rows), :]
        send_ref[i * rows : (i + 1) * rows, :] = total_ref[pl.ds(other, rows), :]


def split_rows(where, total):
    n, d = total.shape
    return pl.pallas_call(
        split_kernel,
        in_specs=[pl.BlockSpec(memory_space=pltpu.SMEM), VMEM],
        out_specs=[VMEM, VMEM],
        out_shape=[pltpu.VMEM((n // 2, d), F32)] * 2,
        cost_estimate=estimate(1 << 20, 4 * n * d * 2),
        compiler_params=pltpu.CompilerParams(vmem_limit_bytes=4 * MIB),
        name="split_rows",
    )(where, *near(total))


def widths_of(columns):
    units = columns // (4 * LANES)
    return [2 * LANES] * (units // 2) + [LANES] * (units % 2)


DUE = {
    "project": -2.5,
    "beside": -1.0,
    "across": 2.0,
    "near": 3.0,
    "far": 4.0,
    "forward": 5.0,
    "stack": 6.0,
    "corner": 8.0,
    "inputs": 8.5,
    "weights": 10.5,
}
LATER = 0.75


def order_of(count):
    due = [(at + LATER * i, i, stage) for i in range(count) for stage, at in DUE.items()]
    return [(stage, i) for _, i, stage in sorted(due, key=lambda entry: entry[:2])]


def halving(tokens, cotangent, gate_weight, up_weight, down_weight):
    return halving_steps(tokens, cotangent, gate_weight, up_weight, down_weight)


def halving_steps(tokens, cotangent, gate_weight, up_weight, down_weight):
    where = jnp.stack(
        [lax.axis_index("depth"), lax.axis_index("col"), lax.axis_index("row")]
    ).astype(jnp.int32)
    first_row = lax.axis_index("row") == 0

    def both(own):
        other = swap(own, "row", 1, 2)
        return jnp.where(
            first_row,
            jnp.concatenate([own, other], axis=0),
            jnp.concatenate([other, own], axis=0),
        )

    tokens_all, cot_all, tokens_t = order_rows(where, both(tokens), both(cotangent))
    n, d = tokens_all.shape
    rows = n // 4
    widths = widths_of(gate_weight.shape[1])
    bases = [4 * sum(widths[:i]) for i in range(len(widths))]
    shapes = (gate_weight.shape, up_weight.shape, down_weight.shape)
    state = {"total": jnp.zeros((n, d), F32), "grads": (), "last": tokens_t}

    def after(*arrays):
        *arrays, _ = lax.optimization_barrier((*arrays, state["last"]))
        return arrays

    def ran(value):
        state["last"] = value

    def piece(base, width):
        def shaped(value, *lead):
            return value.reshape(*lead, 3, rows, width)

        def send(value, axis, mask):
            return swap(value, axis, mask, 4)

        yield
        (t,) = after(tokens_all)
        kept, sent = project(where, t, cot_all, gate_weight, up_weight, down_weight, base, width)
        ran(sent)
        got = send(sent, "col", 1)
        yield
        kept, got = after(kept, got)
        kept, sent = halve(kept, got, 4)
        ran(sent)
        got = send(sent, "col", 2)
        yield
        kept, got = after(kept, got)
        kept, sent = halve(shaped(kept, 4), shaped(got, 4), 2)
        ran(sent)
        got = send(sent, "depth", 1)
        yield
        kept, got = after(kept, got)
        kept, sent = halve(shaped(kept, 2), shaped(got, 2), 1)
        ran(sent)
        got = send(sent, "depth", 2)
        yield
        kept, got = after(kept, got)
        mine = gate_rule(shaped(kept), shaped(got))
        ran(mine)
        second = send(mine, "depth", 2)
        first = send(mine, "depth", 1)
        yield
        (second,) = after(second)
        ran(second)
        third = send(second, "depth", 1)
        yield
        mine, first, second, third = after(mine, first, second, third)
        own = stack_blocks(mine, first, second, third)
        ran(own)
        across = send(own, "col", 2)
        beside = send(own, "col", 1)
        yield
        (across,) = after(across)
        ran(across)
        corner = send(across, "col", 1)
        yield
        own, beside, across, corner = after(own, beside, across, corner)
        shares = (own, beside, across, corner)
        state["total"] = input_part(where, shares, gate_weight, up_weight, state["total"], base, width)
        ran(state["total"])
        yield
        own, beside, across, corner = after(own, beside, across, corner)
        shares = (own, beside, across, corner)
        state["grads"] = weight_part(where, shares, tokens_t, cot_all, state["grads"], shapes, base, width)
        ran(state["grads"][0])

    pieces = [piece(base, width) for base, width in zip(bases, widths)]
    for running in pieces:
        next(running)
    for _, i in order_of(len(pieces)):
        next(pieces[i], None)

    keep, send = split_rows(where, state["total"])
    input_grad = (keep + swap(send, "row", 1, 2)).astype(BF16)
    return (input_grad, *state["grads"])


def fits(sizes, n_tokens, columns):
    mesh_fits = (sizes["depth"], sizes["row"], sizes["col"]) == (4, 2, 4)
    return mesh_fits and n_tokens % 64 == 0 and columns % (4 * LANES) == 0


def solution(mesh):
    sizes = dict(mesh.shape)

    def step(tokens, cotangent, gate_weight, up_weight, down_weight):
        args = (tokens, cotangent, gate_weight, up_weight, down_weight)
        columns = gate_weight.shape[1] // sizes["row"]
        halves = fits(sizes, tokens.shape[0], columns)
        mapped = jax.shard_map(
            halving if halves else stationary,
            mesh=mesh,
            in_specs=(
                P("row", ("depth", "col")),
                P("row", ("depth", "col")),
                P(("depth", "col"), "row"),
                P(("depth", "col"), "row"),
                P("row", ("depth", "col")),
            ),
            out_specs=(
                P("row", ("depth", "col")),
                P(("depth", "col"), "row"),
                P(("depth", "col"), "row"),
                P("row", ("depth", "col")),
            ),
            check_vma=False,
        )
        return mapped(*args)

    return step
```
